64 devices in a mesh: batch: 4 (over x, y), dap: 16 (over z, core).
Axes of the slice: x: 2, y: 2, z: 8, core: 2. Of those that a mesh axis runs over, the one named last changes fastest.
The devices are a block of a 4x4x8 slice.
Arguments:
- pair: bfloat16 [1536, 384, 128], P(('batch', 'dap')), parts along dimension 0
- pair_mask: int32 [1536, 384], P(('batch', 'dap')), parts along dimension 0
- ln_in: bfloat16 [2, 2, 128], replicated
- w_proj: bfloat16 [2, 128, 512], replicated
- b_proj: bfloat16 [2, 512], replicated
- w_gate: bfloat16 [2, 128, 128], replicated
- b_gate: bfloat16 [2, 128], replicated
- ln_out: bfloat16 [2, 2, 128], replicated
- w_out: bfloat16 [2, 128, 128], replicated
- b_out: bfloat16 [2, 128], replicated
Outputs:
- output: bfloat16 [1536, 384, 128], P(('batch', 'dap')), parts along dimension 0
There are 4 independent parts. The reference program is written for one: setup_inputs(seed, part) draws one part's arguments, and reference() takes and returns one part's arrays. A program takes and returns all parts, laid end to end along the dimension named above; an argument that names none is the same for every part.
All inputs are finite; a program needn't handle non-finite values.
Results may differ from the reference program's by a relative error of at most 0.00397731.
Values are sent between devices in bfloat16 or wider.
A program may use at most 768 MiB of HBM per device.

```python
import jax
import jax.numpy as jnp
from jax import lax

N = 384
CZ = 128
CH = 128
LN_EPS = 1e-5


def setup_inputs(seed: int = 0, part: int = 0) -> dict:
    base_key = jax.random.key(seed)
    part_key = jax.random.fold_in(base_key, part)
    pair_key, mask_key = jax.random.split(part_key)
    weight_keys = jax.random.split(jax.random.fold_in(base_key, 1000), 10)
    pair = jax.random.normal(pair_key, (N, N, CZ), jnp.float32)
    pair_mask = (jax.random.randint(mask_key, (N, N), 0, 8) > 0).astype(jnp.int32)
    ln_in = jnp.stack([1.0 + 0.3 * jax.random.normal(weight_keys[0], (2, CZ), jnp.float32),
                       0.3 * jax.random.normal(weight_keys[1], (2, CZ), jnp.float32)], axis=1)
    w_proj = jax.random.normal(weight_keys[2], (2, CZ, 4 * CH), jnp.float32) * CZ ** -0.5
    b_proj = 0.5 * jax.random.normal(weight_keys[3], (2, 4 * CH), jnp.float32)
    w_gate = jax.random.normal(weight_keys[4], (2, CZ, CZ), jnp.float32) * CZ ** -0.5
    b_gate = 0.5 * jax.random.normal(weight_keys[5], (2, CZ), jnp.float32)
    ln_out = jnp.stack([1.0 + 0.3 * jax.random.normal(weight_keys[6], (2, CH), jnp.float32),
                        0.3 * jax.random.normal(weight_keys[7], (2, CH), jnp.float32)], axis=1)
    w_out = jax.random.normal(weight_keys[8], (2, CH, CZ), jnp.float32) * CH ** -0.5
    b_out = 0.5 * jax.random.normal(weight_keys[9], (2, CZ), jnp.float32)
    return {
        "pair": pair.astype(jnp.bfloat16),
        "pair_mask": pair_mask,
        "ln_in": ln_in.astype(jnp.bfloat16),
        "w_proj": w_proj.astype(jnp.bfloat16),
        "b_proj": b_proj.astype(jnp.bfloat16),
        "w_gate": w_gate.astype(jnp.bfloat16),
        "b_gate": b_gate.astype(jnp.bfloat16),
        "ln_out": ln_out.astype(jnp.bfloat16),
        "w_out": w_out.astype(jnp.bfloat16),
        "b_out": b_out.astype(jnp.bfloat16),
    }


def layer_norm(values, scale, offset):
    centred = values - jnp.mean(values, axis=-1, keepdims=True)
    variance = jnp.mean(centred * centred, axis=-1, keepdims=True)
    return centred * lax.rsqrt(variance + LN_EPS) * scale.astype(jnp.float32) + offset.astype(jnp.float32)


def channel_product(left, right, contract_form):
    groups = CH // 16
    left_groups = jnp.moveaxis(left.reshape(N, N, groups, 16), 2, 0)
    right_groups = jnp.moveaxis(right.reshape(N, N, groups, 16), 2, 0)

    def group_sum(operands):
        return jnp.einsum(contract_form, operands[0].astype(jnp.float32), operands[1].astype(jnp.float32))

    summed = lax.map(group_sum, (left_groups, right_groups))
    return jnp.moveaxis(summed, 0, 2).reshape(N, N, CH)


def tri_layer(pair, keep_mask, ln_in, w_proj, b_proj, w_gate, b_gate, ln_out, w_out, b_out, contract_form):
    row_blocks = N // 8

    def make_sides(operands):
        block, mask_block = operands
        normed = layer_norm(block.astype(jnp.float32), ln_in[0], ln_in[1]).astype(jnp.bfloat16)
        projected = jnp.dot(normed.reshape(8 * N, CZ), w_proj, preferred_element_type=jnp.float32)
        projected = (projected + b_proj.astype(jnp.float32)).reshape(8, N, 4 * CH)
        left = mask_block * jax.nn.sigmoid(projected[..., CH:2 * CH]) * projected[..., :CH]
        right = mask_block * jax.nn.sigmoid(projected[..., 3 * CH:]) * projected[..., 2 * CH:3 * CH]
        return normed, left.astype(jnp.bfloat16), right.astype(jnp.bfloat16)

    pair_blocks = pair.reshape(row_blocks, 8, N, CZ)
    normed, left, right = lax.map(make_sides, (pair_blocks, keep_mask.reshape(row_blocks, 8, N, 1)))
    tri_sum = channel_product(left.reshape(N, N, CH), right.reshape(N, N, CH), contract_form)

    def finish(operands):
        block, normed_block, tri_block = operands
        tri_norm = layer_norm(tri_block, ln_out[0], ln_out[1]).astype(jnp.bfloat16)
        update = jnp.dot(tri_norm.reshape(8 * N, CH), w_out, preferred_element_type=jnp.float32) + b_out.astype(jnp.float32)
        gates = jax.nn.sigmoid(jnp.dot(normed_block.reshape(8 * N, CZ), w_gate, preferred_element_type=jnp.float32) + b_gate.astype(jnp.float32))
        return (block.astype(jnp.float32) + (gates * update).reshape(8, N, CZ)).astype(jnp.bfloat16)

    result = lax.map(finish, (pair_blocks, normed, tri_sum.reshape(row_blocks, 8, N, CH)))
    return result.reshape(N, N, CZ)


def reference(pair, pair_mask, ln_in, w_proj, b_proj, w_gate, b_gate, ln_out, w_out, b_out):
    keep_mask = pair_mask.astype(jnp.float32)[..., None]
    first = tri_layer(pair, keep_mask, ln_in[0], w_proj[0], b_proj[0], w_gate[0], b_gate[0],
                      ln_out[0], w_out[0], b_out[0], "ikc,jkc->ijc")
    return tri_layer(first, keep_mask, ln_in[1], w_proj[1], b_proj[1], w_gate[1], b_gate[1],
                     ln_out[1], w_out[1], b_out[1], "kic,kjc->ijc")
```

```python
import functools

import jax
import jax.numpy as jnp
from jax import lax
from jax.experimental import pallas as pl
from jax.experimental.pallas import tpu as pltpu
from jax.sharding import PartitionSpec as P

LN_EPS = 1e-5
F32 = jnp.float32
BF16 = jnp.bfloat16
ROWS = 8


def mm(left, right):
    return jnp.dot(left, right, preferred_element_type=F32)


def norm_first(values, scale, offset):
    centred = values - jnp.mean(values, axis=0, keepdims=True)
    variance = jnp.mean(centred * centred, axis=0, keepdims=True)
    return centred * lax.rsqrt(variance + LN_EPS) * scale + offset


def with_bias_row(normed, mask_row):
    width = normed.shape[1]
    first = lax.broadcasted_iota(jnp.int32, (16, width), 0) == 0
    tail = jnp.where(first, jnp.broadcast_to(mask_row, (16, width)), 0.0).astype(BF16)
    zeros = jnp.zeros((112, width), BF16)
    return jnp.concatenate([(normed * mask_row).astype(BF16), tail, zeros], axis=0)


def gated(projected):
    half = projected.shape[0] // 2
    return (jnp.tanh(projected[half:]) + 1.0) * projected[:half]


def spread(store, block, row, values):
    for c in range(store.shape[1]):
        store[block, c, pl.ds(pl.multiple_of(row * 16, 16), 16), :] = values[16 * c:16 * (c + 1)]


def prep_kernel(devices, chunks, z_ref, m_ref, out_ref):
    for q in range(ROWS):
        x = z_ref[q].astype(F32)
        width, channels = x.shape
        x = x.reshape(devices, chunks, ROWS, channels)
        x = jnp.concatenate([x[:, t].reshape(width // chunks, channels) for t in range(chunks)], axis=0)
        out_ref[channels * q:channels * (q + 1), :] = x.T.astype(BF16)
    masks = m_ref[...]
    out_ref[channels * ROWS:, :] = jnp.concatenate([masks, jnp.zeros_like(masks)], axis=0).astype(BF16)


def sides_kernel(core_ref, z_ref, wa_ref, wb_ref, scale_ref, offset_ref, perm_ref,
                 a_ref, b_ref, normed_ref, keep, spread_b, spread_a):
    channels = a_ref.shape[0]
    core = core_ref[0]

    def mask_of(device):
        return z_ref[device, channels * ROWS:channels * ROWS + 2 * ROWS, :].astype(F32)

    def one_b(device, carry):
        masks = mask_of(device)
        for q in range(ROWS):
            x = z_ref[device, channels * q:channels * (q + 1), :].astype(F32)
            normed = norm_first(x, scale_ref[...], offset_ref[...]).astype(BF16)
            keep[device * ROWS + q] = normed
            rhs = with_bias_row(normed.astype(F32), masks[q:q + 1])
            spread(spread_b, device // 2, (device % 2) * ROWS + q, gated(mm(wb_ref[...], rhs)).astype(BF16))
        return carry

    def one_a(chip, carry):
        device = 2 * chip + core
        masks = mask_of(device)
        for q in range(ROWS):
            normed = keep[device * ROWS + q]
            normed_ref[chip * ROWS + q] = normed
            rhs = with_bias_row(normed.astype(F32), masks[q:q + 1])
            spread(spread_a, 0, chip * ROWS + q, gated(mm(wa_ref[...], rhs)).astype(BF16))
        return carry

    lax.fori_loop(0, 4, one_b, 0)
    lax.fori_loop(0, 2, one_a, 0)
    width = b_ref.shape[2]
    for c in range(channels // 16):
        for chip in range(2):
            b_ref[16 * c:16 * (c + 1), 16 * chip:16 * (chip + 1), :] = (
                mm(perm_ref[...], spread_b[chip, c]).reshape(16, 16, width).astype(BF16))
        a_ref[16 * c:16 * (c + 1)] = mm(perm_ref[...], spread_a[0, c]).reshape(16, 16, width).astype(BF16)


def outgoing_kernel(chunks, *refs):
    a_refs, b_refs, o_ref = refs[:chunks], refs[chunks:2 * chunks], refs[-1]
    for c in range(o_ref.shape[0]):
        left = jnp.concatenate([ref[c] for ref in a_refs], axis=0)
        right = jnp.concatenate([ref[c] for ref in b_refs], axis=0)
        o_ref[c] = lax.dot_general(left, right, (((1,), (1,)), ((), ())), preferred_element_type=F32)


def channel_norm(o_ref, scale_ref, offset_ref, store, group):
    channels, rows, width = o_ref.shape

    def load(c):
        return o_ref[pl.ds(c * group, group)]

    total = lax.fori_loop(0, channels // group, lambda c, s: s + jnp.sum(load(c), axis=0),
                          jnp.zeros((rows, width), F32))
    mean = total * (1.0 / channels)

    def square(c, s):
        d = load(c) - mean[None]
        return s + jnp.sum(d * d, axis=0)

    variance = lax.fori_loop(0, channels // group, square, jnp.zeros((rows, width), F32)) * (1.0 / channels)
    scaled = lax.rsqrt(variance + LN_EPS)

    def write(c, carry):
        d = (load(c) - mean[None]) * scaled[None]
        u = d * scale_ref[pl.ds(c * group, group)] + offset_ref[pl.ds(c * group, group)]
        store[c] = u.reshape(group * rows, width).astype(BF16)
        return carry

    lax.fori_loop(0, channels // group, write, 0)


def middle_kernel(place_ref, o_ref, normed_ref, z_ref, no_scale_ref, no_offset_ref, perm_ref, wo_ref, bo_ref, wg_ref, bg_ref,
                  scale_ref, offset_ref, wa_ref, wb_ref, a_ref, b_ref, z1_ref, store, rows_u, spread_a, spread_b):
    channels, rows, width = o_ref.shape
    core, chip = place_ref[0], place_ref[1]
    chips = pl.num_programs(0) * 2
    lanes = 128
    tiles = width // lanes
    channel_norm(o_ref, no_scale_ref, no_offset_ref, store, 16)
    for c in range(channels // 16):
        rows_u[:, 16 * c:16 * (c + 1), :] = mm(perm_ref[...], store[c]).reshape(rows, 16, width).astype(BF16)
    segment = lanes // chips
    lane = lax.broadcasted_iota(jnp.int32, (1, lanes), 1)

    def pick(x):
        parts = []
        for t in range(tiles):
            shift = lax.rem(t * segment - chip * segment + lanes, lanes)
            parts.append(pltpu.roll(x[:, t * lanes:(t + 1) * lanes], shift, 1))
        out = parts[-1]
        for t in reversed(range(tiles - 1)):
            out = jnp.where(lane < (t + 1) * segment, parts[t], out)
        return out

    for half in range(2):
        masks = z_ref[half, 0, channels * ROWS:channels * ROWS + 2 * ROWS, :].astype(F32)
        for q in range(ROWS):
            i = half * ROWS + q
            update = mm(wo_ref[...], rows_u[i]) + bo_ref[...]
            gates = jnp.tanh(mm(wg_ref[...], normed_ref[i]) + bg_ref[...]) + 1.0
            z = z_ref[half, 0, channels * q:channels * (q + 1), :].astype(F32)
            z1 = (z + gates * update).astype(BF16)

            @pl.when(pl.program_id(0) * 2 + half == chip)
            def _():
                z1_ref[q] = z1

            normed = norm_first(z1.astype(F32), scale_ref[...], offset_ref[...]).astype(BF16).astype(F32)
            mask = masks[q:q + 1]
            spread(spread_b, 0, i, gated(mm(wb_ref[...], with_bias_row(normed, mask))).astype(BF16))
            mask_picked = pick(jnp.broadcast_to(mask, (8, width)))[0:1]
            spread(spread_a, 0, i, gated(mm(wa_ref[...], with_bias_row(pick(normed), mask_picked))).astype(BF16))
    for c in range(channels // 16):
        b_ref[16 * c:16 * (c + 1)] = mm(perm_ref[...], spread_b[0, c]).reshape(16, rows, width).astype(BF16)
        a_ref[16 * c:16 * (c + 1)] = mm(perm_ref[...], spread_a[0, c]).reshape(16, rows, lanes).astype(BF16)


def incoming_kernel(chunks, core_ref, *refs):
    a_refs, b_refs, (own_ref, other_ref, whole) = refs[:chunks], refs[chunks:2 * chunks], refs[-3:]
    core = core_ref[0]
    for c in range(own_ref.shape[0]):
        left = jnp.concatenate([ref[c] for ref in a_refs], axis=0)
        right = jnp.concatenate([ref[c] for ref in b_refs], axis=0)
        whole[c] = lax.dot_general(left, right, (((0,), (0,)), ((), ())), preferred_element_type=F32)
        for t in range(chunks):
            rows = pl.ds(t * ROWS, ROWS)
            own_ref[c, rows, :] = whole[c, pl.ds(pl.multiple_of((2 * t + core) * ROWS, ROWS), ROWS), :]
            other_ref[c, rows, :] = whole[c, pl.ds(pl.multiple_of((2 * t + 1 - core) * ROWS, ROWS), ROWS), :]


def last_kernel(devices, own_ref, got_ref, z1_ref, no_scale_ref, no_offset_ref, perm_ref, wo_ref, bo_ref, wg_ref, bg_ref,
                scale_ref, offset_ref, out_ref, total, store, rows_u):
    channels, rows, width = own_ref.shape
    total[...] = own_ref[...] + got_ref[...]
    channel_norm(total, no_scale_ref, no_offset_ref, store, 32)
    for c in range(channels // 32):
        rows_u[:, 32 * c:32 * (c + 1), :] = mm(perm_ref[...], store[c]).reshape(rows, 32, width).astype(BF16)
    chunks = width // (devices * ROWS)
    for q in range(rows):
        z1 = z1_ref[q].astype(F32)
        normed = norm_first(z1, scale_ref[...], offset_ref[...]).astype(BF16)
        update = mm(wo_ref[...], rows_u[q]) + bo_ref[...]
        gates = jnp.tanh(mm(wg_ref[...], normed) + bg_ref[...]) + 1.0
        z2 = (z1 + gates * update).T.reshape(chunks, devices, ROWS, channels)
        z2 = jnp.concatenate([z2[:, d].reshape(chunks * ROWS, channels) for d in range(devices)], axis=0)
        out_ref[q] = z2.astype(BF16)


def spec(block, index):
    return pl.BlockSpec(block, index)


def whole(array):
    return pl.BlockSpec(array.shape, lambda *_: (0,) * array.ndim)


def swap_order(major, minor):
    row = jnp.arange(major * minor)
    source = (row % major) * minor + row // major
    return (source[:, None] == row[None, :]).astype(BF16)


def call(kernel, name, flops, moved, **kw):
    return pl.pallas_call(kernel, name=name,
                          cost_estimate=pl.CostEstimate(flops=flops, bytes_accessed=moved, transcendentals=0),
                          compiler_params=pltpu.CompilerParams(vmem_limit_bytes=60 * 2**20), **kw)


def solution(mesh):
    row_spec = P(("batch", "dap"), None, None)
    mask_spec = P(("batch", "dap"), None)
    devices = mesh.shape["dap"]
    chips = devices // 2

    def local_layers(pair, pair_mask, ln_in, w_proj, b_proj, w_gate, b_gate, ln_out, w_out, b_out):
        mine, width, channels = pair.shape
        chunks = mine // ROWS
        deep = channels * ROWS + 2 * ROWS
        index = lax.axis_index("dap")
        core, chip = lax.rem(index, 2), index // 2
        place = jnp.stack([core, chip]).astype(jnp.int32)

        mask = pair_mask.astype(F32).reshape(mine, devices, chunks, ROWS).transpose(0, 2, 1, 3).reshape(mine, width)
        packed = []
        for t in range(chunks):
            packed.append(call(
                functools.partial(prep_kernel, devices, chunks), "prep", 10**6, 10**6,
                grid=(1,),
                in_specs=[spec((ROWS, width, channels), lambda s, t=t: (t, 0, 0)), spec((ROWS, width), lambda s, t=t: (t, 0))],
                out_specs=spec((deep, width), lambda s: (0, 0)),
                out_shape=jax.ShapeDtypeStruct((deep, width), BF16))(pair, mask))
        gathered = [lax.all_gather(part, "dap", axis=0, tiled=True).reshape(devices, deep, width) for part in packed]

        def lanes(vector):
            return jnp.broadcast_to(vector.astype(F32)[:, None], (channels, width))

        def planes(vector):
            return jnp.broadcast_to(vector.astype(F32)[:, None, None], (channels, 1, width))

        def side(layer, at):
            w = w_proj[layer][:, 2 * at * channels:2 * (at + 1) * channels].T * BF16(0.5)
            bias = b_proj[layer][2 * at * channels:2 * (at + 1) * channels, None] * BF16(0.5)
            return jnp.concatenate([w, bias, jnp.zeros((2 * channels, channels - 1), BF16)], axis=1)

        wa = [side(layer, 0) for layer in range(2)]
        wb = [side(layer, 1) for layer in range(2)]
        wo = [w_out[layer].T * BF16(0.5) for layer in range(2)]
        wg = [w_gate[layer].T * BF16(0.5) for layer in range(2)]
        bo = [lanes(b_out[layer]) * 0.5 for layer in range(2)]
        bg = [lanes(b_gate[layer]) * 0.5 for layer in range(2)]
        scale_in = [lanes(ln_in[layer, 0]) for layer in range(2)]
        offset_in = [lanes(ln_in[layer, 1]) for layer in range(2)]
        scale_out = [planes(ln_out[layer, 0]) for layer in range(2)]
        offset_out = [planes(ln_out[layer, 1]) for layer in range(2)]
        perm16 = swap_order(16, 16)
        perm_last = swap_order(32, 8)

        chunk_rows = devices * ROWS
        half_rows = chips * ROWS
        steps = devices // 4
        a1, b1, normed1 = [], [], []
        for t in range(chunks):
            consts = [wa[0], wb[0], scale_in[0], offset_in[0], perm16]
            a, b, n = call(
                sides_kernel, "sides", 10**10, 10**8,
                grid_spec=pltpu.PrefetchScalarGridSpec(
                    num_scalar_prefetch=1, grid=(steps,),
                    in_specs=[spec((4, deep, width), lambda s, *_: (s, 0, 0))] + [whole(x) for x in consts],
                    out_specs=[spec((channels, 2 * ROWS, width), lambda s, *_: (0, s, 0)),
                               spec((channels, 4 * ROWS, width), lambda s, *_: (0, s, 0)),
                               spec((2 * ROWS, channels, width), lambda s, *_: (s, 0, 0))],
                    scratch_shapes=[pltpu.VMEM((4 * ROWS, channels, width), BF16),
                                    pltpu.VMEM((2, channels // 16, 256, width), BF16),
                                    pltpu.VMEM((1, channels // 16, 256, width), BF16)]),
                out_shape=[jax.ShapeDtypeStruct((channels, half_rows, width), BF16),
                           jax.ShapeDtypeStruct((channels, chunk_rows, width), BF16),
                           jax.ShapeDtypeStruct((half_rows, channels, width), BF16)])(place, gathered[t], *consts)
            a1.append(a)
            b1.append(b)
            normed1.append(n)

        some = 4
        o1 = call(
            functools.partial(outgoing_kernel, chunks), "outgoing", 10**10, 10**8,
            grid=(channels // some,),
            in_specs=[spec((some, half_rows, width), lambda s: (s, 0, 0))] * chunks
            + [spec((some, chunk_rows, width), lambda s: (s, 0, 0))] * chunks,
            out_specs=spec((some, chunks * half_rows, width), lambda s: (s, 0, 0)),
            out_shape=jax.ShapeDtypeStruct((channels, chunks * half_rows, width), F32))(*a1, *b1)

        a2, b2, z1 = [], [], []
        steps = half_rows // 16
        for t in range(chunks):
            consts = [scale_out[0], offset_out[0], perm16, wo[0], bo[0], wg[0], bg[0],
                      scale_in[1], offset_in[1], wa[1], wb[1]]
            by_core = gathered[t].reshape(chips, 2, deep, width)
            a, b, z = call(
                middle_kernel, "middle", 10**10, 10**8,
                grid_spec=pltpu.PrefetchScalarGridSpec(
                    num_scalar_prefetch=1, grid=(steps,),
                    in_specs=[spec((channels, 16, width), lambda s, place, t=t: (0, t * steps + s, 0)),
                              spec((16, channels, width), lambda s, place: (s, 0, 0)),
                              spec((2, 1, deep, width), lambda s, place: (s, place[0], 0, 0))]
                    + [whole(x) for x in consts],
                    out_specs=[spec((channels, 16, 128), lambda s, *_: (0, s, 0)),
                               spec((channels, 16, width), lambda s, *_: (0, s, 0)),
                               spec((ROWS, channels, width), lambda s, *_: (0, 0, 0))],
                    scratch_shapes=[pltpu.VMEM((channels // 16, 256, width), BF16),
                                    pltpu.VMEM((16, channels, width), BF16),
                                    pltpu.VMEM((1, channels // 16, 256, 128), BF16),
                                    pltpu.VMEM((1, channels // 16, 256, width), BF16)]),
                out_shape=[jax.ShapeDtypeStruct((channels, half_rows, 128), BF16),
                           jax.ShapeDtypeStruct((channels, half_rows, width), BF16),
                           jax.ShapeDtypeStruct((ROWS, channels, width), BF16)])(place, o1, normed1[t], by_core, *consts)
            a2.append(a)
            b2.append(b)
            z1.append(z)

        some = 8
        own, other = call(
            functools.partial(incoming_kernel, chunks), "incoming", 10**10, 10**8,
            grid_spec=pltpu.PrefetchScalarGridSpec(
                num_scalar_prefetch=1, grid=(channels // some,),
                in_specs=[spec((some, half_rows, 128), lambda s, *_: (s, 0, 0))] * chunks
                + [spec((some, half_rows, width), lambda s, *_: (s, 0, 0))] * chunks,
                out_specs=[spec((some, mine, width), lambda s, *_: (s, 0, 0))] * 2,
                scratch_shapes=[pltpu.VMEM((some, 128, width), F32)]),
            out_shape=[jax.ShapeDtypeStruct((channels, mine, width), F32)] * 2)(place, *a2, *b2)
        got = lax.ppermute(other, "dap", [(d, d ^ 1) for d in range(devices)])

        consts = [scale_out[1], offset_out[1], perm_last, wo[1], bo[1], wg[1], bg[1], scale_in[1], offset_in[1]]
        z1 = jnp.concatenate(z1, axis=0)
        return call(
            functools.partial(last_kernel, devices), "last", 10**9, 10**7,
            grid=(chunks,),
            in_specs=[spec((channels, ROWS, width), lambda s: (0, s, 0))] * 2
            + [spec((ROWS, channels, width), lambda s: (s, 0, 0))] + [whole(x) for x in consts],
            out_specs=spec((ROWS, width, channels), lambda s: (s, 0, 0)),
            out_shape=jax.ShapeDtypeStruct(pair.shape, BF16),
            scratch_shapes=[pltpu.VMEM((channels, ROWS, width), F32),
                            pltpu.VMEM((channels // 32, 256, width), BF16),
                            pltpu.VMEM((ROWS, channels, width), BF16)])(own, got, z1, *consts)

    return jax.shard_map(local_layers, mesh=mesh,
                         in_specs=(row_spec, mask_spec, P(), P(), P(), P(), P(), P(), P(), P()),
                         out_specs=row_spec, check_vma=False)
```
